32 devices in a mesh: rows: 16 (over z, y, x), cols: 2 (over core).
Axes of the slice: x: 2, y: 2, z: 4, core: 2. Of those that a mesh axis runs over, the one named last changes fastest.
Arguments:
- panel: float32 [2048, 32768], P('rows', 'cols'), may hold values from -0.03125 to 0.03125
- solved: float32 [32768, 64], P('cols'), may hold values from -6 to 6
- sketch: float32 [2048, 64], P('rows'), may hold values from -6 to 6
- inverses: float32 [2, 1024, 1024], P(None, 'rows', 'cols'), may hold values from -2 to 2, as said below
- coupling: float32 [1024, 1024], P('rows', 'cols'), may hold values from -0.1875 to 0.1875
- design: bfloat16 [32768, 2048], P('rows', 'cols'), may hold values from -0.125 to 0.125
- prior: float32 [32768, 64], P(('rows', 'cols')), may hold values from -6 to 6
Outputs:
- block_solution: float32 [2048, 64], P('rows')
- leverage: float32 [32768], P(('rows', 'cols'))
The draws below stay inside these ranges and needn't reach their ends.
Inputs may be any that keep to these rules, and one draw needn't show every extreme that they name: `inverses`: each of the two blocks is upper triangular with a positive diagonal.
All inputs are finite; a program needn't handle non-finite values.
Results may differ from the reference program's by a relative error of at most 0.00063.
Values sent between devices are 32-bit elements; how exact they have to be, the bound alone decides.
A program may use at most 64 MiB of HBM per device.

```python
import jax
import jax.numpy as jnp
from jax import lax

K = 64
B = 1024
TAIL = 32768
MDEV = 2048
M = 32768
N_ROWS = 16


def draw_inverses(key, part):
    first, second = jax.random.split(jax.random.fold_in(key, 11))
    upper = jnp.clip(jax.random.normal(first, (2, B, B), jnp.float32), -4.0, 4.0)
    upper = upper / jnp.sqrt(jnp.float32(B))
    diagonal = jnp.exp(jax.random.uniform(second, (2, B), jnp.float32, -0.7, 0.4))
    index_row = jax.lax.broadcasted_iota(jnp.int32, (B, B), 0)
    index_col = jax.lax.broadcasted_iota(jnp.int32, (B, B), 1)
    strict = (index_col > index_row).astype(jnp.float32)
    same = (index_col == index_row).astype(jnp.float32)
    return upper * strict[None] + diagonal[:, :, None] * same[None]


def levels(stream_key, dims, shards, low, high):
    gain, own = 1.0, jax.random.fold_in(stream_key, 6)
    for axis_at, parts in shards:
        heights = jnp.exp(jax.random.uniform(jax.random.fold_in(own, axis_at), (parts,), jnp.float32, low / len(shards), high / len(shards)))
        gain = gain * jnp.repeat(heights, dims[axis_at] // parts).reshape([-1 if axis == axis_at else 1 for axis in range(len(dims))])
    return gain


def noise(key, dims, deviation, limit, pieces=(), held_as=jnp.bfloat16):
    values = deviation * jax.random.normal(key, dims, jnp.float32)
    if pieces:
        values = values * levels(key, dims, pieces, -0.22, 0.18)
    return jnp.clip(values, -limit, limit).astype(held_as)


def setup_inputs(seed: int = 0) -> dict:
    key_of = jax.random.split(jax.random.key(seed), 8)
    return {
        "panel": noise(key_of[0], (2 * B, TAIL), TAIL ** -0.5, 0.03125, ((0, 16), (1, 2)), jnp.float32),
        "solved": noise(key_of[1], (TAIL, K), 1.0, 6.0, ((0, 2),), jnp.float32),
        "sketch": noise(key_of[2], (2 * B, K), 1.0, 6.0, ((0, 16),), jnp.float32),
        "inverses": draw_inverses(jax.random.fold_in(key_of[7], 71), 0),
        "coupling": noise(key_of[4], (B, B), B ** -0.5, 0.1875, ((0, 16), (1, 2)), jnp.float32),
        "design": noise(key_of[5], (M, 2 * B), (2 * B) ** -0.5, 0.125, ((0, 16), (1, 2))),
        "prior": noise(key_of[6], (M, K), 1.0, 6.0, ((0, 32),), jnp.float32),
    }


def reference(panel, solved, sketch, inverses, coupling, design, prior):
    highest = lax.Precision.HIGHEST
    right = sketch - jnp.dot(panel, solved, precision=highest)
    y_last = jnp.dot(inverses[1], right[B:], precision=highest)
    bent = jnp.dot(coupling, y_last, precision=highest)
    y_first = jnp.dot(inverses[0], right[:B] - bent, precision=highest)
    block_solution = jnp.concatenate([y_first, y_last], axis=0)
    rounded = block_solution.astype(jnp.bfloat16).astype(jnp.float32)
    stacked = design.reshape(N_ROWS, MDEV, 2 * B)

    def one_block(rows_block):
        return jnp.dot(rows_block.astype(jnp.float32), rounded, precision=highest)

    product = prior + lax.map(one_block, stacked).reshape(N_ROWS * MDEV, K)
    leverage = jnp.mean(product * product, axis=1)
    return block_solution, leverage
```

```python
import functools

import jax
import jax.numpy as jnp
from jax import lax
from jax.experimental import pallas as pl
from jax.experimental.pallas import tpu as pltpu
from jax.sharding import PartitionSpec as P

CHUNKS = 8
EARLY = 3
NT = (((1,), (1,)), ((), ()))


def nt(a, b, precision=None):
    return lax.dot_general(a, b, NT, precision=precision, preferred_element_type=jnp.float32)


def split(x):
    high = x.astype(jnp.bfloat16)
    low = (x - high.astype(jnp.float32)).astype(jnp.bfloat16)
    return jnp.concatenate([high, low], axis=0)


def kernel(
    n,
    panel, solved, sketch, inverses, coupling, design, prior,
    out_solution, out_leverage,
    panel_v, solved_v, sketch_v, design_v, prior_v,
    acc, part_tx, part_rx, right_tx, right_last, right_first,
    w_rx, w_split, y_tx, y_last, z_tx, z_all, s_tx, y_first,
    y_half, prod_tx, prod_rx, sol_tx, sol_rx, lev_tx, lev_rx,
    load_sem, w_send, w_recv, send_sem, pair_send, recv_sem,
):
    r = lax.axis_index("rows")
    c = lax.axis_index("cols")
    peer = 1 - c
    q = n // 4
    plane, p = r // q, r % q
    bottom, upper = plane // 2, plane % 2
    depth = panel.shape[1]
    step = depth // CHUNKS
    k, pr = sketch.shape
    ir = pr // 2
    width = inverses.shape[2]
    rows_here = prior.shape[1]

    def chunk(i):
        at = pl.ds(pl.multiple_of(i * step, step), step)
        return (
            pltpu.make_async_copy(panel.at[:, at], panel_v.at[:, at], load_sem.at[0, i]),
            pltpu.make_async_copy(solved.at[:, at], solved_v.at[:, at], load_sem.at[1, i]),
        )

    for i in range(CHUNKS):
        for copy in chunk(i):
            copy.start()
    late = [
        pltpu.make_async_copy(src, dst, load_sem.at[2, i])
        for i, (src, dst) in enumerate(((sketch, sketch_v), (prior, prior_v), (design, design_v)))
    ]

    barrier = pltpu.get_barrier_semaphore()

    def greet(to, core):
        pl.semaphore_signal(
            barrier, inc=1, device_id=(to, core), device_id_type=pl.DeviceIdType.MESH
        )

    @pl.when(c == 0)
    def _():
        greet(r, 1)

    @pl.when(c == 1)
    def _():
        def column(i, carry):
            greet(i * q + p, 0)
            return carry

        def others(i, carry):
            greet((r + 1 + i) % n, 1)
            return carry

        lax.fori_loop(0, 4, column, 0)
        lax.fori_loop(0, n - 1, others, 0)

    acc[...] = jnp.zeros_like(acc)

    def body(i, carry):
        for copy in chunk(i):
            copy.wait()
        at = pl.ds(pl.multiple_of(i * step, step), step)
        acc[...] += nt(split(solved_v[:, at]), split(panel_v[:, at]))
        return carry

    def remote(src, dst, to, core, sent, recv):
        return pltpu.make_async_remote_copy(
            src_ref=src,
            dst_ref=dst,
            send_sem=sent,
            recv_sem=recv,
            device_id=(to, core),
            device_id_type=pl.DeviceIdType.MESH,
        )

    def put(src, dst, to, core, sent, recv):
        here = jnp.logical_and(to == r, core == c)

        @pl.when(here)
        def _():
            pltpu.make_async_copy(src, dst, recv).start()

        @pl.when(jnp.logical_not(here))
        def _():
            remote(src, dst, to, core, sent, recv).start()

    def settle(src, dst, to, core, sent, recv):
        here = jnp.logical_and(to == r, core == c)

        @pl.when(jnp.logical_not(here))
        def _():
            remote(src, dst, to, core, sent, recv).wait_send()

    def arrived(ref, recv):
        pltpu.make_async_copy(ref, ref, recv).wait()

    def weights(act, which):
        src = (inverses.at[1], coupling, inverses.at[0])[which]
        rows_at = pl.ds(pl.multiple_of(ir * upper, ir), ir)

        def move(skip):
            size = width - skip
            cols_at = pl.ds(pl.multiple_of(width * c + skip, skip or width), size)
            act(
                src.at[:, skip:],
                w_rx.at[which, rows_at, cols_at],
                (1 + bottom) * q + p,
                1,
                w_send.at[which],
                w_recv.at[which, upper, c],
            )

        if which == 1:
            move(0)
        else:

            @pl.when(jnp.logical_and(c == bottom, upper == 1))
            def _():
                move(width // 2)

            @pl.when(jnp.logical_or(c > bottom, jnp.logical_and(c == bottom, upper == 0)))
            def _():
                move(0)

    def bulk():
        weights(put, 0)
        weights(put, 1)

    early = jnp.logical_or(c == 0, plane >= 2)

    def meet():
        pl.semaphore_wait(barrier, jnp.where(c == 0, 4, n))
        bulk()

    late[0].start()
    lax.fori_loop(0, EARLY, body, 0)
    pl.when(early)(meet)
    lax.fori_loop(EARLY, CHUNKS, body, 0)
    pl.when(jnp.logical_not(early))(meet)
    total = acc[...]
    part = (total[:k, :pr] + total[k:, :pr]) + (total[:k, pr:] + total[k:, pr:])

    def to_peer(src, dst, which, recv):
        return remote(src, dst, r, peer, pair_send.at[which], recv_sem.at[recv])

    part_copy = to_peer(part_tx, part_rx, 0, 3)
    prod_copies = [
        to_peer(
            prod_tx.at[:, i * rows_here : (i + 1) * rows_here],
            prod_rx.at[:, i * rows_here : (i + 1) * rows_here],
            1 + i,
            8,
        )
        for i in range(2)
    ]
    sol_copy = to_peer(sol_tx, sol_rx, 3, 9)
    lev_copy = to_peer(lev_tx, lev_rx, 4, 10)

    lane = lax.broadcasted_iota(jnp.int32, (k, pr), 1)

    def fold(a, b, odd):
        even_half = jnp.where(lane < ir, a, pltpu.roll(b, ir, 1))
        odd_half = jnp.where(lane < ir, pltpu.roll(a, ir, 1), b)
        return jnp.where(odd, odd_half, even_half)

    def natural(ref, t):
        at = (t // q) * q + (2 * t) % q
        a = ref[:, pl.ds(pl.multiple_of(at * pr, pr), pr)]
        b = ref[:, pl.ds(pl.multiple_of((at + 1) * pr, pr), pr)]
        return fold(a, b, (t % q) // (q // 2) == 1)

    def whole(ref):
        for t in range(2 * q):
            at = (t // q) * q + (2 * t) % q
            a = ref[:, at * pr : (at + 1) * pr]
            b = ref[:, (at + 1) * pr : (at + 2) * pr]
            if (t % q) // (q // 2) == 1:
                both = jnp.where(lane < ir, pltpu.roll(a, ir, 1), b)
            else:
                both = jnp.where(lane < ir, a, pltpu.roll(b, ir, 1))
            y_half[:, t * pr : (t + 1) * pr] = both.astype(jnp.bfloat16)

    def product(which):
        return nt(y_half[...], design_v[which * rows_here : (which + 1) * rows_here, :])

    def piece(h):
        return pl.ds(pl.multiple_of((h * q + p) * pr, pr), pr)

    def near(i):
        return (p + 1 + i) % q

    def spread(act, count, src, dst, where, core, phase, recv):
        def one(i, carry):
            act(src, dst, where(i), core, send_sem.at[phase, i], recv_sem.at[recv])
            return carry

        lax.fori_loop(0, count, one, 0)

    last_args = (right_tx, right_last.at[:, pl.ds(pl.multiple_of(pr * (r % (2 * q)), pr), pr)])

    def spread_last(act):
        def where(i):
            return (1 + i // q) * q + near(i)

        @pl.when(plane == 3)
        def _():
            spread(act, 2 * q, *last_args, where, 1, 0, 4)

        @pl.when(plane == 2)
        def _():
            spread(act, q, *last_args, where, 1, 0, 4)

    def spread_first(act):
        @pl.when(plane < 2)
        def _():
            for i in range(2):
                j = 2 * r + i
                to = (1 + j // (2 * q)) * q + j % q
                act(right_tx, right_first.at[(j % (2 * q)) // q], to, 1, send_sem.at[0, i], recv_sem.at[5])

    def spread_y_last(act):
        def where(i):
            s = i // q
            return jnp.where(s == 0, 3 - plane, jnp.where(s == 1, plane, 3 * s - 6)) * q + near(i)

        spread(act, n, y_tx, y_last.at[:, piece(bottom)], where, 1, 1, 6)

    def spread_z(act):
        @pl.when(plane == 2)
        def _():
            spread(act, 2 * q, z_tx, z_all.at[:, piece(1)], lambda i: (1 + i // q) * q + near(i), 1, 2, 7)

        @pl.when(plane == 1)
        def _():
            spread(act, q, z_tx, z_all.at[:, piece(0)], lambda i: q + near(i), 1, 2, 7)

    def spread_y_first(act):
        def where(i):
            return (i // q) * q + near(i)

        spread(act, n, s_tx, y_first.at[:, piece(bottom)], where, 0, 3, 11)

    def prepare(which, lo):
        size = 2 * width - lo
        x = w_rx[which, :, lo:]
        if which:
            wide = lax.broadcasted_iota(jnp.int32, (pr, pr), 1)
            blocks = []
            for base in range(0, size, width):
                for at in range(q):
                    i = base + (at // 2) * pr
                    j = i + width // 2
                    a, b = x[:, i : i + pr], x[:, j : j + pr]
                    if at % 2:
                        blocks.append(jnp.where(wide < ir, pltpu.roll(a, ir, 1), b))
                    else:
                        blocks.append(jnp.where(wide < ir, a, pltpu.roll(b, ir, 1)))
            x = jnp.concatenate(blocks, axis=1)
        w_split[which, :, lo:] = split(x)

    def ready(which, lo):
        skip = width // 2 if which != 1 else 0
        if skip:
            w_rx[which, ir:, lo : lo + skip] = jnp.zeros((ir, skip), jnp.float32)
        for core in range(lo // width, 2):
            for up in range(2):
                first = width * core + (skip if up == 1 and width * core == lo else 0)
                arrived(
                    w_rx.at[which, ir * up : ir * up + ir, first : width * core + width],
                    w_recv.at[which, up, core],
                )
        prepare(which, lo)

    def times(ref, which, lo):
        terms = nt(split(ref[:, lo:]), w_split[which, :, lo:])
        terms = terms[:k] + terms[k:]
        return terms[:, :pr] + terms[:, pr:]

    @pl.when(c == 0)
    def _():
        part_tx[...] = part
        part_copy.start()
        weights(put, 2)
        late[1].start()
        late[2].start()
        late[0].wait()
        late[1].wait()
        late[2].wait()
        arrived(prod_rx, recv_sem.at[8])
        prod_tx[:, :rows_here] = prod_rx[:, :rows_here] + prior_v[...]
        arrived(y_first, recv_sem.at[11])
        whole(y_first)
        theirs = product(1) + prod_rx[:, rows_here:]
        lev_tx[...] = jnp.mean(theirs * theirs, axis=0, keepdims=True)
        lev_copy.start()

        @pl.when(plane < 2)
        def _():
            mine = natural(y_first, r % (2 * q))
            sol_tx[...] = mine
            sol_copy.start()
            out_solution[...] = mine

        ours = product(0) + prod_tx[:, :rows_here]
        out_leverage[...] = jnp.mean(ours * ours, axis=0, keepdims=True)

        @pl.when(plane >= 2)
        def _():
            arrived(sol_rx, recv_sem.at[9])
            out_solution[...] = sol_rx[...]

        @pl.when(plane < 2)
        def _():
            sol_copy.wait_send()

        part_copy.wait_send()
        lev_copy.wait_send()

    @pl.when(c == 1)
    def _():
        late[0].wait()
        own = sketch_v[...] - part
        arrived(part_rx, recv_sem.at[3])
        right_tx[...] = own - part_rx[...]
        spread_last(put)
        spread_first(put)
        weights(put, 2)
        late[1].start()
        late[2].start()

        def solve(lo):
            ready(0, lo)
            arrived(right_last.at[:, lo:], recv_sem.at[4])
            y_tx[...] = times(right_last, 0, lo)
            arrived(right_first, recv_sem.at[5])
            spread_y_last(put)
            z_tx[...] = fold(right_first[0], right_first[1], p % 2 == 1)
            ready(1, 0)
            arrived(y_last, recv_sem.at[6])
            z_tx[...] = z_tx[...] - times(y_last, 1, 0)
            spread_z(put)
            ready(2, lo)
            arrived(z_all.at[:, lo:], recv_sem.at[7])
            s_tx[...] = times(z_all, 2, lo)
            spread_y_first(put)

        @pl.when(plane == 1)
        def _():
            solve(0)

        @pl.when(plane == 2)
        def _():
            solve(width)

        inner = jnp.logical_or(plane == 1, plane == 2)

        @pl.when(jnp.logical_not(inner))
        def _():
            arrived(y_last, recv_sem.at[6])

        late[1].wait()
        late[2].wait()
        whole(y_last)
        prod_tx[:, :rows_here] = product(0)
        prod_copies[0].start()
        prod_tx[:, rows_here:] = product(1) + prior_v[...]
        prod_copies[1].start()

        @pl.when(plane >= 2)
        def _():
            mine = natural(y_last, r % (2 * q))
            sol_tx[...] = mine
            sol_copy.start()
            out_solution[...] = mine

        spread_last(settle)
        spread_first(settle)

        @pl.when(inner)
        def _():
            spread_y_last(settle)
            spread_z(settle)
            spread_y_first(settle)

        for copy in prod_copies:
            copy.wait_send()

        @pl.when(plane >= 2)
        def _():
            sol_copy.wait_send()

        @pl.when(plane < 2)
        def _():
            arrived(sol_rx, recv_sem.at[9])
            out_solution[...] = sol_rx[...]

        arrived(lev_rx, recv_sem.at[10])
        out_leverage[...] = lev_rx[...]

    for which in range(3):
        weights(settle, which)


def pinned(x):
    return pltpu.with_memory_space_constraint(x, pltpu.HBM)


def fused(n, panel, solved, sketch, inverses, coupling, design, prior):
    k = sketch.shape[1]
    pr, depth = panel.shape
    rows_here = prior.shape[0]
    width = inverses.shape[2]
    f32 = jnp.float32
    out_solution, out_leverage = pl.pallas_call(
        functools.partial(kernel, n),
        out_shape=(
            jax.ShapeDtypeStruct((k, pr), f32),
            jax.ShapeDtypeStruct((1, rows_here), f32),
        ),
        in_specs=[pl.BlockSpec(memory_space=pltpu.HBM)] * 7,
        out_specs=[pl.BlockSpec(memory_space=pltpu.VMEM)] * 2,
        scratch_shapes=[
            pltpu.VMEM((pr, depth), f32),
            pltpu.VMEM((k, depth), f32),
            pltpu.VMEM((k, pr), f32),
            pltpu.VMEM(design.shape, design.dtype),
            pltpu.VMEM((k, rows_here), f32),
            pltpu.VMEM((2 * k, 2 * pr), f32),
            pltpu.VMEM((k, pr), f32),
            pltpu.VMEM((k, pr), f32),
            pltpu.VMEM((k, pr), f32),
            pltpu.VMEM((k, 2 * width), f32),
            pltpu.VMEM((2, k, pr), f32),
            pltpu.VMEM((3, pr, 2 * width), f32),
            pltpu.VMEM((3, 2 * pr, 2 * width), jnp.bfloat16),
            pltpu.VMEM((k, pr), f32),
            pltpu.VMEM((k, 2 * width), f32),
            pltpu.VMEM((k, pr), f32),
            pltpu.VMEM((k, 2 * width), f32),
            pltpu.VMEM((k, pr), f32),
            pltpu.VMEM((k, 2 * width), f32),
            pltpu.VMEM((k, 2 * width), jnp.bfloat16),
            pltpu.VMEM((k, 2 * rows_here), f32),
            pltpu.VMEM((k, 2 * rows_here), f32),
            pltpu.VMEM((k, pr), f32),
            pltpu.VMEM((k, pr), f32),
            pltpu.VMEM((1, rows_here), f32),
            pltpu.VMEM((1, rows_here), f32),
            pltpu.SemaphoreType.DMA((3, CHUNKS)),
            pltpu.SemaphoreType.DMA((3,)),
            pltpu.SemaphoreType.DMA((3, 2, 2)),
            pltpu.SemaphoreType.DMA((4, n)),
            pltpu.SemaphoreType.DMA((5,)),
            pltpu.SemaphoreType.DMA((12,)),
        ],
        compiler_params=pltpu.CompilerParams(
            collective_id=0, has_side_effects=True, vmem_limit_bytes=28 * 1024 * 1024
        ),
    )(*map(pinned, (panel, solved.T, sketch.T, inverses, coupling, design, prior.T)))
    return out_solution.T, out_leverage.reshape(rows_here)


def assemble(term):
    rows_here = lax.psum(term, "cols")
    return lax.all_gather(rows_here, "rows", axis=0, tiled=True)


def local(panel, solved, sketch, inverses, coupling, design, prior):
    highest = lax.Precision.HIGHEST
    partial_value = jnp.dot(panel, solved, precision=highest)
    local_right = sketch - lax.psum(partial_value, "cols")
    right = lax.all_gather(local_right, "rows", axis=0, tiled=True)
    blocks = right.shape[0] // 2
    width = inverses.shape[2]
    column = lax.axis_index("cols")
    offset = column * width

    def piece(vector):
        return lax.dynamic_slice_in_dim(vector, offset, width, 0)

    right_first = right[:blocks]
    right_last = right[blocks:]
    sketch_cols = right.shape[1]
    inverse_full = lax.all_gather(inverses[0], "cols", axis=1, tiled=True)
    coupling_full = lax.all_gather(coupling, "rows", axis=0, tiled=True)
    mixed = jnp.dot(inverse_full, coupling_full, precision=highest)
    term_last = jnp.dot(inverses[1], piece(right_last), precision=highest)
    term_first = jnp.dot(inverses[0], piece(right_first), precision=highest)
    joined = assemble(jnp.concatenate([term_last, term_first], axis=1))
    y_last = joined[:, :sketch_cols]
    partial_first = joined[:, sketch_cols:]
    correction = assemble(jnp.dot(mixed, piece(y_last), precision=highest))
    y_first = partial_first - correction
    solution = jnp.concatenate([y_first, y_last], axis=0)
    own_rows = sketch.shape[0]
    block_solution = lax.dynamic_slice_in_dim(
        solution, lax.axis_index("rows") * own_rows, own_rows, 0
    )
    design_cols = design.shape[1]
    rounded = lax.dynamic_slice_in_dim(solution, column * design_cols, design_cols, 0).astype(
        jnp.bfloat16
    )
    mine = lax.psum_scatter(
        jnp.dot(design, rounded, preferred_element_type=jnp.float32),
        "cols",
        scatter_dimension=0,
        tiled=True,
    )
    product = prior + mine
    leverage = jnp.mean(product * product, axis=1)
    return (block_solution, leverage)


def local_or_fused(rows, panel, solved, sketch, inverses, coupling, design, prior):
    args = (panel, solved, sketch, inverses, coupling, design, prior)
    pr, depth = panel.shape
    fits = pr == 128 and depth % (CHUNKS * 128) == 0 and sketch.shape[1] % 32 == 0
    return fused(rows, *args) if fits else local(*args)


def solution(mesh):
    in_specs = (
        P("rows", "cols"),
        P("cols", None),
        P("rows", None),
        P(None, "rows", "cols"),
        P("rows", "cols"),
        P("rows", "cols"),
        P(("rows", "cols"), None),
    )
    out_specs = (P("rows", None), P(("rows", "cols")))
    rows, cols = mesh.shape["rows"], mesh.shape["cols"]
    step = local
    if cols == 2 and rows % 8 == 0:
        step = functools.partial(local_or_fused, rows)
    return jax.shard_map(step, mesh=mesh, in_specs=in_specs, out_specs=out_specs, check_vma=False)
```

```python
import functools

import jax
import jax.numpy as jnp
from jax import lax
from jax.experimental import pallas as pl
from jax.experimental.pallas import tpu as pltpu
from jax.sharding import PartitionSpec as P

CHUNKS = 8
EARLY = 3
PARTS = 1
SLABS = 4
NT = (((1,), (1,)), ((), ()))


def nt(a, b, precision=None):
    return lax.dot_general(a, b, NT, precision=precision, preferred_element_type=jnp.float32)


def split(x):
    high = x.astype(jnp.bfloat16)
    low = (x - high.astype(jnp.float32)).astype(jnp.bfloat16)
    return jnp.concatenate([high, low], axis=0)


def kernel(
    n,
    panel, solved, sketch, inverses, coupling, design, prior,
    out_solution, out_leverage,
    panel_v, solved_v, sketch_v, design_v, prior_v,
    acc, part_tx, part_rx, right_tx, right_last, right_first,
    w_rx, w_split, y_tx, y_last, z_tx, z_all, s_tx, y_first,
    y_half, prod_tx, prod_rx, held, sol_tx, sol_rx, wide, design_own,
    load_sem, w_send, w_recv, send_sem, pair_send, recv_sem, wide_send, wide_recv,
):
    r = lax.axis_index("rows")
    c = lax.axis_index("cols")
    peer = 1 - c
    q = n // 4
    plane, p = r // q, r % q
    bottom, upper = plane // 2, plane % 2
    depth = panel.shape[1]
    step = depth // CHUNKS
    k, pr = sketch.shape
    ir = pr // 2
    kh = k // PARTS
    width = inverses.shape[2]
    rows_here = prior.shape[1]

    def chunk(i):
        at = pl.ds(pl.multiple_of(i * step, step), step)
        return (
            pltpu.make_async_copy(panel.at[:, at], panel_v.at[:, at], load_sem.at[0, i]),
            pltpu.make_async_copy(solved.at[:, at], solved_v.at[:, at], load_sem.at[1, i]),
        )

    for i in range(CHUNKS):
        for copy in chunk(i):
            copy.start()
    late = [
        pltpu.make_async_copy(src, dst, load_sem.at[2, i])
        for i, (src, dst) in enumerate(((sketch, sketch_v), (prior, prior_v), (design, design_v)))
    ]

    barrier = pltpu.get_barrier_semaphore()

    def greet(to, core):
        pl.semaphore_signal(
            barrier, inc=1, device_id=(to, core), device_id_type=pl.DeviceIdType.MESH
        )

    @pl.when(c == 0)
    def _():
        greet(r, 1)

    @pl.when(c == 1)
    def _():
        def column(i, carry):
            greet(i * q + p, 0)
            return carry

        def others(i, carry):
            greet((r + 1 + i) % n, 1)
            return carry

        lax.fori_loop(0, 4, column, 0)
        lax.fori_loop(0, n - 1, others, 0)

    acc[...] = jnp.zeros_like(acc)

    def body(i, carry):
        for copy in chunk(i):
            copy.wait()
        at = pl.ds(pl.multiple_of(i * step, step), step)
        acc[...] += nt(split(solved_v[:, at]), split(panel_v[:, at]))
        return carry

    def remote(src, dst, to, core, sent, recv):
        return pltpu.make_async_remote_copy(
            src_ref=src,
            dst_ref=dst,
            send_sem=sent,
            recv_sem=recv,
            device_id=(to, core),
            device_id_type=pl.DeviceIdType.MESH,
        )

    def put(src, dst, to, core, sent, recv):
        here = jnp.logical_and(to == r, core == c)

        @pl.when(here)
        def _():
            pltpu.make_async_copy(src, dst, recv).start()

        @pl.when(jnp.logical_not(here))
        def _():
            remote(src, dst, to, core, sent, recv).start()

    def settle(src, dst, to, core, sent, recv):
        here = jnp.logical_and(to == r, core == c)

        @pl.when(jnp.logical_not(here))
        def _():
            remote(src, dst, to, core, sent, recv).wait_send()

    def arrived(ref, recv):
        pltpu.make_async_copy(ref, ref, recv).wait()

    def weights(act, which):
        src = (inverses.at[1], coupling, inverses.at[0])[which]
        rows_at = pl.ds(pl.multiple_of(ir * upper, ir), ir)

        def move(skip):
            size = width - skip
            cols_at = pl.ds(pl.multiple_of(width * c + skip, skip or width), size)
            act(
                src.at[:, skip:],
                w_rx.at[which, rows_at, cols_at],
                (1 + bottom) * q + p,
                1,
                w_send.at[which],
                w_recv.at[which, upper, c],
            )

        if which == 1:
            move(0)
        else:

            @pl.when(jnp.logical_and(c == bottom, upper == 1))
            def _():
                move(width // 2)

            @pl.when(jnp.logical_or(c > bottom, jnp.logical_and(c == bottom, upper == 0)))
            def _():
                move(0)

    def bulk():
        weights(put, 0)
        weights(put, 1)

    early = jnp.logical_or(c == 0, plane >= 2)

    def meet():
        pl.semaphore_wait(barrier, jnp.where(c == 0, 4, n))
        bulk()

    late[0].start()
    lax.fori_loop(0, EARLY, body, 0)
    pl.when(early)(meet)
    lax.fori_loop(EARLY, CHUNKS, body, 0)
    pl.when(jnp.logical_not(early))(meet)
    total = acc[...]
    share = (total[:k, :pr] + total[k:, :pr]) + (total[:k, pr:] + total[k:, pr:])

    def to_peer(src, dst, which, recv):
        return remote(src, dst, r, peer, pair_send.at[which], recv_sem.at[recv, 0])

    part_copy = to_peer(part_tx, part_rx, 0, 3)
    prod_copy = to_peer(prod_tx, prod_rx, 1, 0)
    sol_copy = to_peer(sol_tx, sol_rx, 2, 1)

    def group(g):
        return slice(g * width, (g + 1) * width)

    passes = [to_peer(y_first.at[:, group(g)], y_first.at[:, group(g)], 3 + g, 9 + g) for g in range(2)]
    slab = rows_here // SLABS

    def widen(i):
        at = pl.ds(pl.multiple_of(slab * i, slab), slab)
        return remote(wide.at[at], wide.at[at], r, 1, wide_send.at[i], wide_recv.at[i])

    lane = lax.broadcasted_iota(jnp.int32, (k, pr), 1)

    def fold(a, b, odd):
        even_half = jnp.where(lane < ir, a, pltpu.roll(b, ir, 1))
        odd_half = jnp.where(lane < ir, pltpu.roll(a, ir, 1), b)
        return jnp.where(odd, odd_half, even_half)

    def natural(ref, t):
        at = (t // q) * q + (2 * t) % q
        a = ref[:, pl.ds(pl.multiple_of(at * pr, pr), pr)]
        b = ref[:, pl.ds(pl.multiple_of((at + 1) * pr, pr), pr)]
        return fold(a, b, (t % q) // (q // 2) == 1)

    def round_group(ref, g):
        for t in range(g * q, (g + 1) * q):
            at = g * q + (2 * t) % q
            a = ref[:, at * pr : (at + 1) * pr]
            b = ref[:, (at + 1) * pr : (at + 2) * pr]
            if (t % q) // (q // 2) == 1:
                both = jnp.where(lane < ir, pltpu.roll(a, ir, 1), b)
            else:
                both = jnp.where(lane < ir, a, pltpu.roll(b, ir, 1))
            y_half[:, t * pr : (t + 1) * pr] = both.astype(jnp.bfloat16)

    def product(which):
        return nt(y_half[...], design_v[which * rows_here : (which + 1) * rows_here, :])

    def finish(g, weights_of):
        round_group(y_first, g)
        held[...] += nt(y_half[:, group(g)], weights_of[:rows_here, group(g)])

    def conclude():
        total_here = held[...]
        out_leverage[...] = jnp.mean(total_here * total_here, axis=0, keepdims=True)

        @pl.when(plane < 2)
        def _():
            out_solution[...] = natural(y_first, r % (2 * q))

    def piece(h):
        return pl.ds(pl.multiple_of((h * q + p) * pr, pr), pr)

    def near(i):
        return (p + 1 + i) % q

    def mixed(i, count):
        planes = count // q
        return (1 + i % planes) * q + near(i // planes)

    def spread(act, span, src, dst, cols_at, where, core, phase, part):
        rows_at = slice(part * kh, (part + 1) * kh)

        def one(i, carry):
            to = where(i // q) * q + near(i) if phase else mixed(i, span[1])
            sent = send_sem.at[phase, part, i]
            recv = recv_sem.at[4 + phase if phase < 3 else 7 + bottom, part]
            act(src.at[rows_at], dst.at[rows_at, cols_at], to, core, sent, recv)
            return carry

        lax.fori_loop(*span, one, 0)

    last_at = pl.ds(pl.multiple_of(pr * (r % (2 * q)), pr), pr)

    def spread_last(act):
        def send(planes):
            for part in range(PARTS):
                spread(act, (0, planes * q), right_tx, right_last, last_at, lambda s: 1 + s, 1, 0, part)

        @pl.when(plane == 3)
        def _():
            send(2)

        @pl.when(plane == 2)
        def _():
            send(1)

    def spread_first(act):
        @pl.when(plane < 2)
        def _():
            for i in range(2):
                j = 2 * r + i
                to = (1 + j // (2 * q)) * q + j % q
                act(right_tx, right_first.at[(j % (2 * q)) // q], to, 1, send_sem.at[0, 0, i], recv_sem.at[2, 0])

    def spread_y_last(act, part, span):
        def where(s):
            return jnp.where(s == 0, 3 - plane, jnp.where(s == 1, plane, 3 * s - 6))

        spread(act, span, y_tx, y_last, piece(bottom), where, 1, 1, part)

    def spread_z(act, part):
        @pl.when(plane == 2)
        def _():
            spread(act, (0, 2 * q), z_tx, z_all, piece(1), lambda s: 1 + s, 1, 2, part)

        @pl.when(plane == 1)
        def _():
            spread(act, (0, q), z_tx, z_all, piece(0), lambda s: 1 + s, 1, 2, part)

    def spread_y_first(act, part):
        spread(act, (0, n), s_tx, y_first, piece(bottom), lambda s: s, 1, 3, part)

    def here(ref, phase, part, lo=0):
        arrived(ref.at[part * kh : (part + 1) * kh, lo:], recv_sem.at[4 + phase, part])

    def prepare(which, lo):
        size = 2 * width - lo
        x = w_rx[which, :, lo:]
        if which:
            wide = lax.broadcasted_iota(jnp.int32, (pr, pr), 1)
            blocks = []
            for base in range(0, size, width):
                for at in range(q):
                    i = base + (at // 2) * pr
                    j = i + width // 2
                    a, b = x[:, i : i + pr], x[:, j : j + pr]
                    if at % 2:
                        blocks.append(jnp.where(wide < ir, pltpu.roll(a, ir, 1), b))
                    else:
                        blocks.append(jnp.where(wide < ir, a, pltpu.roll(b, ir, 1)))
            x = jnp.concatenate(blocks, axis=1)
        w_split[which, :, lo:] = split(x)

    def ready(which, lo):
        skip = width // 2 if which != 1 else 0
        if skip:
            w_rx[which, ir:, lo : lo + skip] = jnp.zeros((ir, skip), jnp.float32)
        for core in range(lo // width, 2):
            for up in range(2):
                first = width * core + (skip if up == 1 and width * core == lo else 0)
                arrived(
                    w_rx.at[which, ir * up : ir * up + ir, first : width * core + width],
                    w_recv.at[which, up, core],
                )
        prepare(which, lo)

    def times(ref, which, part, lo):
        terms = nt(split(ref[part * kh : (part + 1) * kh, lo:]), w_split[which, :, lo:])
        terms = terms[:kh] + terms[kh:]
        return terms[:, :pr] + terms[:, pr:]

    @pl.when(c == 0)
    def _():
        part_tx[...] = share
        part_copy.start()
        weights(put, 2)
        late[1].start()
        late[2].start()
        late[0].wait()
        late[1].wait()
        late[2].wait()

        def share_slab(i, carry):
            at = pl.ds(pl.multiple_of(slab * i, slab), slab)
            theirs = pl.ds(pl.multiple_of(rows_here + slab * i, slab), slab)
            wide[at, :] = design_v[theirs, :].astype(jnp.float32)
            widen(i).start()
            return carry

        lax.fori_loop(0, SLABS, share_slab, 0)
        arrived(prod_rx, recv_sem.at[0, 0])
        held[...] = prod_rx[...] + prior_v[...]

        @pl.when(plane >= 2)
        def _():
            arrived(sol_rx, recv_sem.at[1, 0])
            out_solution[...] = sol_rx[...]

        for g in (1, 0):
            arrived(y_first.at[:, group(g)], recv_sem.at[9 + g, 0])
            finish(g, design_v)
        conclude()
        part_copy.wait_send()

        def sent_slab(i, carry):
            widen(i).wait_send()
            return carry

        lax.fori_loop(0, SLABS, sent_slab, 0)

    @pl.when(c == 1)
    def _():
        late[0].wait()
        own = sketch_v[...] - share
        arrived(part_rx, recv_sem.at[3, 0])
        right_tx[...] = own - part_rx[...]
        spread_last(put)
        spread_first(put)
        weights(put, 2)
        late[1].start()
        late[2].start()

        def solve(lo):
            ready(0, lo)
            for part in range(PARTS):
                here(right_last, 0, part, lo)
                y_tx[part * kh : (part + 1) * kh] = times(right_last, 0, part, lo)
                spread_y_last(put, part, (0, 2 * q))
            for part in range(PARTS):
                spread_y_last(put, part, (2 * q, n))
            ready(1, 0)
            arrived(right_first, recv_sem.at[2, 0])
            z_tx[...] = fold(right_first[0], right_first[1], p % 2 == 1)
            for part in range(PARTS):
                at = slice(part * kh, (part + 1) * kh)
                here(y_last, 1, part)
                z_tx[at] = z_tx[at] - times(y_last, 1, part, 0)
                spread_z(put, part)
            ready(2, lo)
            for part in range(PARTS):
                here(z_all, 2, part, lo)
                s_tx[part * kh : (part + 1) * kh] = times(z_all, 2, part, lo)
                spread_y_first(put, part)

        @pl.when(plane == 1)
        def _():
            solve(0)

        @pl.when(plane == 2)
        def _():
            solve(width)

        inner = jnp.logical_or(plane == 1, plane == 2)

        @pl.when(jnp.logical_not(inner))
        def _():
            for part in range(PARTS):
                here(y_last, 1, part)

        late[1].wait()
        late[2].wait()
        for g in range(2):
            round_group(y_last, g)
        prod_tx[...] = product(0)
        prod_copy.start()
        held[...] = product(1) + prior_v[...]

        @pl.when(plane >= 2)
        def _():
            mine = natural(y_last, r % (2 * q))
            sol_tx[...] = mine
            sol_copy.start()
            out_solution[...] = mine

        def narrow_slab(i, carry):
            at = pl.ds(pl.multiple_of(slab * i, slab), slab)
            arrived(wide.at[at], wide_recv.at[i])
            design_own[at, :] = wide[at, :].astype(jnp.bfloat16)
            return carry

        lax.fori_loop(0, SLABS, narrow_slab, 0)
        for g in (1, 0):
            arrived(y_first.at[:, group(g)], recv_sem.at[7 + g, 0])
            passes[g].start()
        for g in (1, 0):
            finish(g, design_own)
        conclude()
        spread_last(settle)
        spread_first(settle)

        @pl.when(inner)
        def _():
            for part in range(PARTS):
                spread_y_last(settle, part, (0, n))
                spread_z(settle, part)
                spread_y_first(settle, part)

        prod_copy.wait_send()
        for copy in passes:
            copy.wait_send()

        @pl.when(plane >= 2)
        def _():
            sol_copy.wait_send()

    for which in range(3):
        weights(settle, which)


def emit(solution_v, leverage_v, out_solution, out_leverage, sem):
    copies = [
        pltpu.make_async_copy(solution_v, out_solution, sem.at[0]),
        pltpu.make_async_copy(leverage_v, out_leverage, sem.at[1]),
    ]
    for copy in copies:
        copy.start()
    for copy in copies:
        copy.wait()


def pinned(x):
    return pltpu.with_memory_space_constraint(x, pltpu.HBM)


def fused(n, panel, solved, sketch, inverses, coupling, design, prior):
    k = sketch.shape[1]
    pr, depth = panel.shape
    rows_here = prior.shape[0]
    width = inverses.shape[2]
    f32 = jnp.float32
    out_solution, out_leverage = pl.pallas_call(
        functools.partial(kernel, n),
        out_shape=(
            jax.ShapeDtypeStruct((k, pr), f32),
            jax.ShapeDtypeStruct((1, rows_here), f32),
        ),
        in_specs=[pl.BlockSpec(memory_space=pltpu.HBM)] * 7,
        out_specs=[pl.BlockSpec(memory_space=pltpu.VMEM)] * 2,
        scratch_shapes=[
            pltpu.VMEM((pr, depth), f32),
            pltpu.VMEM((k, depth), f32),
            pltpu.VMEM((k, pr), f32),
            pltpu.VMEM(design.shape, design.dtype),
            pltpu.VMEM((k, rows_here), f32),
            pltpu.VMEM((2 * k, 2 * pr), f32),
            pltpu.VMEM((k, pr), f32),
            pltpu.VMEM((k, pr), f32),
            pltpu.VMEM((k, pr), f32),
            pltpu.VMEM((k, 2 * width), f32),
            pltpu.VMEM((2, k, pr), f32),
            pltpu.VMEM((3, pr, 2 * width), f32),
            pltpu.VMEM((3, 2 * pr, 2 * width), jnp.bfloat16),
            pltpu.VMEM((k, pr), f32),
            pltpu.VMEM((k, 2 * width), f32),
            pltpu.VMEM((k, pr), f32),
            pltpu.VMEM((k, 2 * width), f32),
            pltpu.VMEM((k, pr), f32),
            pltpu.VMEM((k, 2 * width), f32),
            pltpu.VMEM((k, 2 * width), jnp.bfloat16),
            pltpu.VMEM((k, rows_here), f32),
            pltpu.VMEM((k, rows_here), f32),
            pltpu.VMEM((k, rows_here), f32),
            pltpu.VMEM((k, pr), f32),
            pltpu.VMEM((k, pr), f32),
            pltpu.VMEM((rows_here, design.shape[1]), f32),
            pltpu.VMEM((rows_here, design.shape[1]), design.dtype),
            pltpu.SemaphoreType.DMA((3, CHUNKS)),
            pltpu.SemaphoreType.DMA((3,)),
            pltpu.SemaphoreType.DMA((3, 2, 2)),
            pltpu.SemaphoreType.DMA((4, PARTS, n)),
            pltpu.SemaphoreType.DMA((5,)),
            pltpu.SemaphoreType.DMA((11, PARTS)),
            pltpu.SemaphoreType.DMA((SLABS,)),
            pltpu.SemaphoreType.DMA((SLABS,)),
        ],
        compiler_params=pltpu.CompilerParams(
            collective_id=0, has_side_effects=True, vmem_limit_bytes=36 * 1024 * 1024
        ),
    )(*map(pinned, (panel, solved.T, sketch.T, inverses, coupling, design, prior.T)))
    out_solution, out_leverage = pl.pallas_call(
        emit,
        out_shape=(
            jax.ShapeDtypeStruct((k, pr), f32),
            jax.ShapeDtypeStruct((1, rows_here), f32),
        ),
        in_specs=[pl.BlockSpec(memory_space=pltpu.VMEM)] * 2,
        out_specs=[pl.BlockSpec(memory_space=pltpu.HBM)] * 2,
        scratch_shapes=[pltpu.SemaphoreType.DMA((2,))],
    )(*(pltpu.with_memory_space_constraint(x, pltpu.VMEM) for x in (out_solution, out_leverage)))
    return out_solution.T, out_leverage.reshape(rows_here)


def assemble(term):
    rows_here = lax.psum(term, "cols")
    return lax.all_gather(rows_here, "rows", axis=0, tiled=True)


def local(panel, solved, sketch, inverses, coupling, design, prior):
    highest = lax.Precision.HIGHEST
    partial_value = jnp.dot(panel, solved, precision=highest)
    local_right = sketch - lax.psum(partial_value, "cols")
    right = lax.all_gather(local_right, "rows", axis=0, tiled=True)
    blocks = right.shape[0] // 2
    width = inverses.shape[2]
    column = lax.axis_index("cols")
    offset = column * width

    def piece(vector):
        return lax.dynamic_slice_in_dim(vector, offset, width, 0)

    right_first = right[:blocks]
    right_last = right[blocks:]
    sketch_cols = right.shape[1]
    inverse_full = lax.all_gather(inverses[0], "cols", axis=1, tiled=True)
    coupling_full = lax.all_gather(coupling, "rows", axis=0, tiled=True)
    mixed = jnp.dot(inverse_full, coupling_full, precision=highest)
    term_last = jnp.dot(inverses[1], piece(right_last), precision=highest)
    term_first = jnp.dot(inverses[0], piece(right_first), precision=highest)
    joined = assemble(jnp.concatenate([term_last, term_first], axis=1))
    y_last = joined[:, :sketch_cols]
    partial_first = joined[:, sketch_cols:]
    correction = assemble(jnp.dot(mixed, piece(y_last), precision=highest))
    y_first = partial_first - correction
    solution = jnp.concatenate([y_first, y_last], axis=0)
    own_rows = sketch.shape[0]
    block_solution = lax.dynamic_slice_in_dim(
        solution, lax.axis_index("rows") * own_rows, own_rows, 0
    )
    design_cols = design.shape[1]
    rounded = lax.dynamic_slice_in_dim(solution, column * design_cols, design_cols, 0).astype(
        jnp.bfloat16
    )
    mine = lax.psum_scatter(
        jnp.dot(design, rounded, preferred_element_type=jnp.float32),
        "cols",
        scatter_dimension=0,
        tiled=True,
    )
    product = prior + mine
    leverage = jnp.mean(product * product, axis=1)
    return (block_solution, leverage)


def local_or_fused(rows, panel, solved, sketch, inverses, coupling, design, prior):
    args = (panel, solved, sketch, inverses, coupling, design, prior)
    pr, depth = panel.shape
    fits = pr == 128 and depth % (CHUNKS * 128) == 0 and sketch.shape[1] % 32 == 0
    return fused(rows, *args) if fits else local(*args)


def solution(mesh):
    in_specs = (
        P("rows", "cols"),
        P("cols", None),
        P("rows", None),
        P(None, "rows", "cols"),
        P("rows", "cols"),
        P("rows", "cols"),
        P(("rows", "cols"), None),
    )
    out_specs = (P("rows", None), P(("rows", "cols")))
    rows, cols = mesh.shape["rows"], mesh.shape["cols"]
    step = local
    if cols == 2 and rows % 8 == 0:
        step = functools.partial(local_or_fused, rows)
    return jax.shard_map(step, mesh=mesh, in_specs=in_specs, out_specs=out_specs, check_vma=False)
```

```python
import functools

import jax
import jax.numpy as jnp
from jax import lax
from jax.experimental import pallas as pl
from jax.experimental.pallas import tpu as pltpu
from jax.sharding import PartitionSpec as P

CHUNKS = 8
EARLY = 4
PARTS = 1
SLABS = 4
NT = (((1,), (1,)), ((), ()))


def nt(a, b, precision=None):
    return lax.dot_general(a, b, NT, precision=precision, preferred_element_type=jnp.float32)


def split(x):
    high = x.astype(jnp.bfloat16)
    low = (x - high.astype(jnp.float32)).astype(jnp.bfloat16)
    return jnp.concatenate([high, low], axis=0)


def kernel(
    n,
    panel, solved, sketch, inverses, coupling, design, prior,
    out_solution, out_leverage,
    panel_v, solved_v, sketch_v, design_v, prior_v,
    acc, part_tx, part_rx, right_tx, right_last, right_first,
    w_rx, w_split, y_tx, y_last, z_tx, z_all, s_tx, y_first,
    y_half, prod_tx, prod_rx, held, sol_tx, sol_rx, wide, design_own,
    load_sem, w_send, w_recv, send_sem, pair_send, recv_sem, wide_send, wide_recv,
):
    r = lax.axis_index("rows")
    c = lax.axis_index("cols")
    peer = 1 - c
    q = n // 4
    plane, p = r // q, r % q
    bottom, upper = plane // 2, plane % 2
    depth = panel.shape[1]
    step = depth // CHUNKS
    k, pr = sketch.shape
    ir = pr // 2
    kh = k // PARTS
    width = inverses.shape[2]
    rows_here = prior.shape[1]

    def chunk(i):
        at = pl.ds(pl.multiple_of(i * step, step), step)
        return (
            pltpu.make_async_copy(panel.at[:, at], panel_v.at[:, at], load_sem.at[0, i]),
            pltpu.make_async_copy(solved.at[:, at], solved_v.at[:, at], load_sem.at[1, i]),
        )

    for i in range(CHUNKS):
        for copy in chunk(i):
            copy.start()
    late = [
        pltpu.make_async_copy(src, dst, load_sem.at[2, i])
        for i, (src, dst) in enumerate(((sketch, sketch_v), (prior, prior_v), (design, design_v)))
    ]

    barrier = pltpu.get_barrier_semaphore()

    def greet(to, core):
        pl.semaphore_signal(
            barrier, inc=1, device_id=(to, core), device_id_type=pl.DeviceIdType.MESH
        )

    @pl.when(c == 0)
    def _():
        greet(r, 1)

        @pl.when(r == 0)
        def _():
            def solvers(i, carry):
                greet(q + i, 1)
                return carry

            lax.fori_loop(0, 2 * q, solvers, 0)

    @pl.when(c == 1)
    def _():
        def column(i, carry):
            greet(i * q + p, 0)
            return carry

        def others(i, carry):
            greet((r + 1 + i) % n, 1)
            return carry

        lax.fori_loop(0, 4, column, 0)
        lax.fori_loop(0, n - 1, others, 0)

    acc[...] = jnp.zeros_like(acc)

    def body(i, carry):
        for copy in chunk(i):
            copy.wait()
        at = pl.ds(pl.multiple_of(i * step, step), step)
        acc[...] += nt(split(solved_v[:, at]), split(panel_v[:, at]))
        return carry

    def remote(src, dst, to, core, sent, recv):
        return pltpu.make_async_remote_copy(
            src_ref=src,
            dst_ref=dst,
            send_sem=sent,
            recv_sem=recv,
            device_id=(to, core),
            device_id_type=pl.DeviceIdType.MESH,
        )

    def put(src, dst, to, core, sent, recv):
        here = jnp.logical_and(to == r, core == c)

        @pl.when(here)
        def _():
            pltpu.make_async_copy(src, dst, recv).start()

        @pl.when(jnp.logical_not(here))
        def _():
            remote(src, dst, to, core, sent, recv).start()

    def settle(src, dst, to, core, sent, recv):
        here = jnp.logical_and(to == r, core == c)

        @pl.when(jnp.logical_not(here))
        def _():
            remote(src, dst, to, core, sent, recv).wait_send()

    def arrived(ref, recv):
        pltpu.make_async_copy(ref, ref, recv).wait()

    def weights(act, which):
        src = (inverses.at[1], coupling, inverses.at[0])[which]
        rows_at = pl.ds(pl.multiple_of(ir * upper, ir), ir)

        def move(skip):
            size = width - skip
            cols_at = pl.ds(pl.multiple_of(width * c + skip, skip or width), size)
            act(
                src.at[:, skip:],
                w_rx.at[which, rows_at, cols_at],
                (1 + bottom) * q + p,
                1,
                w_send.at[which],
                w_recv.at[which, upper, c],
            )

        if which == 1:
            move(0)
        else:

            @pl.when(jnp.logical_and(c == bottom, upper == 1))
            def _():
                move(width // 2)

            @pl.when(jnp.logical_or(c > bottom, jnp.logical_and(c == bottom, upper == 0)))
            def _():
                move(0)

    def bulk():
        weights(put, 0)
        weights(put, 1)

    early = jnp.logical_or(c == 0, plane >= 2)
    inner = jnp.logical_or(plane == 1, plane == 2)

    def meet():
        pl.semaphore_wait(barrier, jnp.where(c == 0, 4, jnp.where(inner, n + 1, n)))
        bulk()

    late[0].start()
    pl.when(plane == 3)(meet)
    lax.fori_loop(0, EARLY, body, 0)
    pl.when(jnp.logical_and(early, plane < 3))(meet)
    lax.fori_loop(EARLY, CHUNKS, body, 0)
    pl.when(jnp.logical_not(early))(meet)
    total = acc[...]
    share = (total[:k, :pr] + total[k:, :pr]) + (total[:k, pr:] + total[k:, pr:])

    def to_peer(src, dst, which, recv):
        return remote(src, dst, r, peer, pair_send.at[which], recv_sem.at[recv, 0])

    part_copy = to_peer(part_tx, part_rx, 0, 3)
    prod_copy = to_peer(prod_tx, prod_rx, 1, 0)
    sol_copy = to_peer(sol_tx, sol_rx, 2, 1)

    def group(g):
        return slice(g * width, (g + 1) * width)

    passes = [to_peer(y_first.at[:, group(g)], y_first.at[:, group(g)], 3 + g, 9 + g) for g in range(2)]
    slab = rows_here // SLABS

    def widen(i):
        at = pl.ds(pl.multiple_of(slab * i, slab), slab)
        return remote(wide.at[at], wide.at[at], r, 1, wide_send.at[i], wide_recv.at[i])

    lane = lax.broadcasted_iota(jnp.int32, (k, pr), 1)

    def fold(a, b, odd):
        even_half = jnp.where(lane < ir, a, pltpu.roll(b, ir, 1))
        odd_half = jnp.where(lane < ir, pltpu.roll(a, ir, 1), b)
        return jnp.where(odd, odd_half, even_half)

    def natural(ref, t):
        at = (t // q) * q + (2 * t) % q
        a = ref[:, pl.ds(pl.multiple_of(at * pr, pr), pr)]
        b = ref[:, pl.ds(pl.multiple_of((at + 1) * pr, pr), pr)]
        return fold(a, b, (t % q) // (q // 2) == 1)

    def round_group(ref, g):
        for t in range(g * q, (g + 1) * q):
            at = g * q + (2 * t) % q
            a = ref[:, at * pr : (at + 1) * pr]
            b = ref[:, (at + 1) * pr : (at + 2) * pr]
            if (t % q) // (q // 2) == 1:
                both = jnp.where(lane < ir, pltpu.roll(a, ir, 1), b)
            else:
                both = jnp.where(lane < ir, a, pltpu.roll(b, ir, 1))
            y_half[:, t * pr : (t + 1) * pr] = both.astype(jnp.bfloat16)

    def product(which):
        return nt(y_half[...], design_v[which * rows_here : (which + 1) * rows_here, :])

    def finish(g, weights_of):
        round_group(y_first, g)
        held[...] += nt(y_half[:, group(g)], weights_of[:rows_here, group(g)])

    def conclude():
        total_here = held[...]
        out_leverage[...] = jnp.mean(total_here * total_here, axis=0, keepdims=True)

        @pl.when(plane < 2)
        def _():
            out_solution[...] = natural(y_first, r % (2 * q))

    def piece(h):
        return pl.ds(pl.multiple_of((h * q + p) * pr, pr), pr)

    def near(i):
        return (p + 1 + i) % q

    def mixed(i, count):
        planes = count // q
        return (1 + i % planes) * q + near(i // planes)

    def spread(act, span, src, dst, cols_at, where, core, phase, part):
        rows_at = slice(part * kh, (part + 1) * kh)

        def one(i, carry):
            to = (mixed(i, span[1]), where(i // q) * q + near(i), where(i // q) * q + near(i), i)[phase]
            sent = send_sem.at[phase, part, i]
            recv = recv_sem.at[4 + phase if phase < 3 else 7 + bottom, part]
            act(src.at[rows_at], dst.at[rows_at, cols_at], to, core, sent, recv)
            return carry

        lax.fori_loop(*span, one, 0)

    last_at = pl.ds(pl.multiple_of(pr * (r % (2 * q)), pr), pr)

    def spread_last(act):
        def send(planes):
            for part in range(PARTS):
                spread(act, (0, planes * q), right_tx, right_last, last_at, lambda s: 1 + s, 1, 0, part)

        @pl.when(plane == 3)
        def _():
            send(2)

        @pl.when(plane == 2)
        def _():
            send(1)

    def spread_first(act):
        @pl.when(plane < 2)
        def _():
            for i in range(2):
                j = 2 * r + i
                to = (1 + j // (2 * q)) * q + j % q
                act(right_tx, right_first.at[(j % (2 * q)) // q], to, 1, send_sem.at[0, 0, i], recv_sem.at[2, 0])

    def spread_y_last(act, part, span):
        def where(s):
            return jnp.where(s == 0, 3 - plane, jnp.where(s == 1, plane, 3 * s - 6))

        spread(act, span, y_tx, y_last, piece(bottom), where, 1, 1, part)

    def spread_z(act, part):
        @pl.when(plane == 2)
        def _():
            spread(act, (0, 2 * q), z_tx, z_all, piece(1), lambda s: 1 + s, 1, 2, part)

        @pl.when(plane == 1)
        def _():
            spread(act, (0, q), z_tx, z_all, piece(0), lambda s: 1 + s, 1, 2, part)

    def spread_y_first(act, part):
        at = piece(bottom)
        act(s_tx, y_first.at[:, at], 0, 0, pair_send.at[5], recv_sem.at[9 + bottom, 0])
        spread(act, (0, n), s_tx, y_first, at, lambda s: s, 1, 3, part)

    def here(ref, phase, part, lo=0):
        arrived(ref.at[part * kh : (part + 1) * kh, lo:], recv_sem.at[4 + phase, part])

    def prepare(which, lo):
        size = 2 * width - lo
        x = w_rx[which, :, lo:]
        if which:
            wide = lax.broadcasted_iota(jnp.int32, (pr, pr), 1)
            blocks = []
            for base in range(0, size, width):
                for at in range(q):
                    i = base + (at // 2) * pr
                    j = i + width // 2
                    a, b = x[:, i : i + pr], x[:, j : j + pr]
                    if at % 2:
                        blocks.append(jnp.where(wide < ir, pltpu.roll(a, ir, 1), b))
                    else:
                        blocks.append(jnp.where(wide < ir, a, pltpu.roll(b, ir, 1)))
            x = jnp.concatenate(blocks, axis=1)
        w_split[which, :, lo:] = split(x)

    def ready(which, lo):
        skip = width // 2 if which != 1 else 0
        if skip:
            w_rx[which, ir:, lo : lo + skip] = jnp.zeros((ir, skip), jnp.float32)
        for core in range(lo // width, 2):
            for up in range(2):
                first = width * core + (skip if up == 1 and width * core == lo else 0)
                arrived(
                    w_rx.at[which, ir * up : ir * up + ir, first : width * core + width],
                    w_recv.at[which, up, core],
                )
        prepare(which, lo)

    def times(ref, which, part, lo):
        terms = nt(split(ref[part * kh : (part + 1) * kh, lo:]), w_split[which, :, lo:])
        terms = terms[:kh] + terms[kh:]
        return terms[:, :pr] + terms[:, pr:]

    @pl.when(c == 0)
    def _():
        part_tx[...] = share
        part_copy.start()
        weights(put, 2)
        late[1].start()
        late[2].start()
        late[0].wait()
        late[1].wait()
        late[2].wait()

        def share_slab(i, carry):
            at = pl.ds(pl.multiple_of(slab * i, slab), slab)
            theirs = pl.ds(pl.multiple_of(rows_here + slab * i, slab), slab)
            wide[at, :] = design_v[theirs, :].astype(jnp.float32)
            widen(i).start()
            return carry

        lax.fori_loop(0, SLABS, share_slab, 0)
        arrived(prod_rx, recv_sem.at[0, 0])
        held[...] = prod_rx[...] + prior_v[...]

        @pl.when(plane >= 2)
        def _():
            arrived(sol_rx, recv_sem.at[1, 0])
            out_solution[...] = sol_rx[...]

        for g in (1, 0):
            arrived(y_first.at[:, group(g)], recv_sem.at[9 + g, 0])
            finish(g, design_v)
        conclude()
        part_copy.wait_send()

        def sent_slab(i, carry):
            widen(i).wait_send()
            return carry

        lax.fori_loop(0, SLABS, sent_slab, 0)

    @pl.when(c == 1)
    def _():
        late[0].wait()
        own = sketch_v[...] - share
        arrived(part_rx, recv_sem.at[3, 0])
        right_tx[...] = own - part_rx[...]
        spread_last(put)
        spread_first(put)
        weights(put, 2)
        late[1].start()
        late[2].start()

        def solve(lo):
            ready(0, lo)
            for part in range(PARTS):
                here(right_last, 0, part, lo)
                y_tx[part * kh : (part + 1) * kh] = times(right_last, 0, part, lo)
                spread_y_last(put, part, (0, 2 * q))
            for part in range(PARTS):
                spread_y_last(put, part, (2 * q, n))
            ready(1, 0)
            arrived(right_first, recv_sem.at[2, 0])
            z_tx[...] = fold(right_first[0], right_first[1], p % 2 == 1)
            for part in range(PARTS):
                at = slice(part * kh, (part + 1) * kh)
                here(y_last, 1, part)
                z_tx[at] = z_tx[at] - times(y_last, 1, part, 0)
                spread_z(put, part)
            ready(2, lo)
            for part in range(PARTS):
                here(z_all, 2, part, lo)
                s_tx[part * kh : (part + 1) * kh] = times(z_all, 2, part, lo)
                spread_y_first(put, part)

        @pl.when(plane == 1)
        def _():
            solve(0)

        @pl.when(plane == 2)
        def _():
            solve(width)

        @pl.when(jnp.logical_not(inner))
        def _():
            for part in range(PARTS):
                here(y_last, 1, part)

        late[1].wait()
        late[2].wait()
        for g in range(2):
            round_group(y_last, g)
        prod_tx[...] = product(0)
        prod_copy.start()
        held[...] = product(1) + prior_v[...]

        @pl.when(plane >= 2)
        def _():
            mine = natural(y_last, r % (2 * q))
            sol_tx[...] = mine
            sol_copy.start()
            out_solution[...] = mine

        def narrow_slab(i, carry):
            at = pl.ds(pl.multiple_of(slab * i, slab), slab)
            arrived(wide.at[at], wide_recv.at[i])
            design_own[at, :] = wide[at, :].astype(jnp.bfloat16)
            return carry

        lax.fori_loop(0, SLABS, narrow_slab, 0)
        for g in (1, 0):
            arrived(y_first.at[:, group(g)], recv_sem.at[7 + g, 0])
            pl.when(r > 0)(passes[g].start)
        for g in (1, 0):
            finish(g, design_own)
        conclude()
        spread_last(settle)
        spread_first(settle)

        @pl.when(inner)
        def _():
            for part in range(PARTS):
                spread_y_last(settle, part, (0, n))
                spread_z(settle, part)
                spread_y_first(settle, part)

        prod_copy.wait_send()
        for copy in passes:
            pl.when(r > 0)(copy.wait_send)

        @pl.when(plane >= 2)
        def _():
            sol_copy.wait_send()

    for which in range(3):
        weights(settle, which)


def emit(solution_v, leverage_v, out_solution, out_leverage, sem):
    copies = [
        pltpu.make_async_copy(solution_v, out_solution, sem.at[0]),
        pltpu.make_async_copy(leverage_v, out_leverage, sem.at[1]),
    ]
    for copy in copies:
        copy.start()
    for copy in copies:
        copy.wait()


def pinned(x):
    return pltpu.with_memory_space_constraint(x, pltpu.HBM)


def fused(n, panel, solved, sketch, inverses, coupling, design, prior):
    k = sketch.shape[1]
    pr, depth = panel.shape
    rows_here = prior.shape[0]
    width = inverses.shape[2]
    f32 = jnp.float32
    out_solution, out_leverage = pl.pallas_call(
        functools.partial(kernel, n),
        out_shape=(
            jax.ShapeDtypeStruct((k, pr), f32),
            jax.ShapeDtypeStruct((1, rows_here), f32),
        ),
        in_specs=[pl.BlockSpec(memory_space=pltpu.HBM)] * 7,
        out_specs=[pl.BlockSpec(memory_space=pltpu.VMEM)] * 2,
        scratch_shapes=[
            pltpu.VMEM((pr, depth), f32),
            pltpu.VMEM((k, depth), f32),
            pltpu.VMEM((k, pr), f32),
            pltpu.VMEM(design.shape, design.dtype),
            pltpu.VMEM((k, rows_here), f32),
            pltpu.VMEM((2 * k, 2 * pr), f32),
            pltpu.VMEM((k, pr), f32),
            pltpu.VMEM((k, pr), f32),
            pltpu.VMEM((k, pr), f32),
            pltpu.VMEM((k, 2 * width), f32),
            pltpu.VMEM((2, k, pr), f32),
            pltpu.VMEM((3, pr, 2 * width), f32),
            pltpu.VMEM((3, 2 * pr, 2 * width), jnp.bfloat16),
            pltpu.VMEM((k, pr), f32),
            pltpu.VMEM((k, 2 * width), f32),
            pltpu.VMEM((k, pr), f32),
            pltpu.VMEM((k, 2 * width), f32),
            pltpu.VMEM((k, pr), f32),
            pltpu.VMEM((k, 2 * width), f32),
            pltpu.VMEM((k, 2 * width), jnp.bfloat16),
            pltpu.VMEM((k, rows_here), f32),
            pltpu.VMEM((k, rows_here), f32),
            pltpu.VMEM((k, rows_here), f32),
            pltpu.VMEM((k, pr), f32),
            pltpu.VMEM((k, pr), f32),
            pltpu.VMEM((rows_here, design.shape[1]), f32),
            pltpu.VMEM((rows_here, design.shape[1]), design.dtype),
            pltpu.SemaphoreType.DMA((3, CHUNKS)),
            pltpu.SemaphoreType.DMA((3,)),
            pltpu.SemaphoreType.DMA((3, 2, 2)),
            pltpu.SemaphoreType.DMA((4, PARTS, n)),
            pltpu.SemaphoreType.DMA((6,)),
            pltpu.SemaphoreType.DMA((11, PARTS)),
            pltpu.SemaphoreType.DMA((SLABS,)),
            pltpu.SemaphoreType.DMA((SLABS,)),
        ],
        compiler_params=pltpu.CompilerParams(
            collective_id=0, has_side_effects=True, vmem_limit_bytes=36 * 1024 * 1024
        ),
    )(*map(pinned, (panel, solved.T, sketch.T, inverses, coupling, design, prior.T)))
    out_solution, out_leverage = pl.pallas_call(
        emit,
        out_shape=(
            jax.ShapeDtypeStruct((k, pr), f32),
            jax.ShapeDtypeStruct((1, rows_here), f32),
        ),
        in_specs=[pl.BlockSpec(memory_space=pltpu.VMEM)] * 2,
        out_specs=[pl.BlockSpec(memory_space=pltpu.HBM)] * 2,
        scratch_shapes=[pltpu.SemaphoreType.DMA((2,))],
    )(*(pltpu.with_memory_space_constraint(x, pltpu.VMEM) for x in (out_solution, out_leverage)))
    return out_solution.T, out_leverage.reshape(rows_here)


def assemble(term):
    rows_here = lax.psum(term, "cols")
    return lax.all_gather(rows_here, "rows", axis=0, tiled=True)


def local(panel, solved, sketch, inverses, coupling, design, prior):
    highest = lax.Precision.HIGHEST
    partial_value = jnp.dot(panel, solved, precision=highest)
    local_right = sketch - lax.psum(partial_value, "cols")
    right = lax.all_gather(local_right, "rows", axis=0, tiled=True)
    blocks = right.shape[0] // 2
    width = inverses.shape[2]
    column = lax.axis_index("cols")
    offset = column * width

    def piece(vector):
        return lax.dynamic_slice_in_dim(vector, offset, width, 0)

    right_first = right[:blocks]
    right_last = right[blocks:]
    sketch_cols = right.shape[1]
    inverse_full = lax.all_gather(inverses[0], "cols", axis=1, tiled=True)
    coupling_full = lax.all_gather(coupling, "rows", axis=0, tiled=True)
    mixed = jnp.dot(inverse_full, coupling_full, precision=highest)
    term_last = jnp.dot(inverses[1], piece(right_last), precision=highest)
    term_first = jnp.dot(inverses[0], piece(right_first), precision=highest)
    joined = assemble(jnp.concatenate([term_last, term_first], axis=1))
    y_last = joined[:, :sketch_cols]
    partial_first = joined[:, sketch_cols:]
    correction = assemble(jnp.dot(mixed, piece(y_last), precision=highest))
    y_first = partial_first - correction
    solution = jnp.concatenate([y_first, y_last], axis=0)
    own_rows = sketch.shape[0]
    block_solution = lax.dynamic_slice_in_dim(
        solution, lax.axis_index("rows") * own_rows, own_rows, 0
    )
    design_cols = design.shape[1]
    rounded = lax.dynamic_slice_in_dim(solution, column * design_cols, design_cols, 0).astype(
        jnp.bfloat16
    )
    mine = lax.psum_scatter(
        jnp.dot(design, rounded, preferred_element_type=jnp.float32),
        "cols",
        scatter_dimension=0,
        tiled=True,
    )
    product = prior + mine
    leverage = jnp.mean(product * product, axis=1)
    return (block_solution, leverage)


def local_or_fused(rows, panel, solved, sketch, inverses, coupling, design, prior):
    args = (panel, solved, sketch, inverses, coupling, design, prior)
    pr, depth = panel.shape
    fits = pr == 128 and depth % (CHUNKS * 128) == 0 and sketch.shape[1] % 32 == 0
    return fused(rows, *args) if fits else local(*args)


def solution(mesh):
    in_specs = (
        P("rows", "cols"),
        P("cols", None),
        P("rows", None),
        P(None, "rows", "cols"),
        P("rows", "cols"),
        P("rows", "cols"),
        P(("rows", "cols"), None),
    )
    out_specs = (P("rows", None), P(("rows", "cols")))
    rows, cols = mesh.shape["rows"], mesh.shape["cols"]
    step = local
    if cols == 2 and rows % 8 == 0:
        step = functools.partial(local_or_fused, rows)
    return jax.shard_map(step, mesh=mesh, in_specs=in_specs, out_specs=out_specs, check_vma=False)
```

```python
import functools

import jax
import jax.numpy as jnp
from jax import lax
from jax.experimental import pallas as pl
from jax.experimental.pallas import tpu as pltpu
from jax.sharding import PartitionSpec as P

CHUNKS = 5
EARLY = 2
PARTS = 1
LEAD = 16
SLABS = 4
NT = (((1,), (1,)), ((), ()))


def nt(a, b, precision=None):
    return lax.dot_general(a, b, NT, precision=precision, preferred_element_type=jnp.float32)


def split(x):
    high = x.astype(jnp.bfloat16)
    low = (x - high.astype(jnp.float32)).astype(jnp.bfloat16)
    return jnp.concatenate([high, low], axis=0)


def kernel(
    n,
    panel, solved, sketch, inverses, coupling, design, prior,
    out_solution, out_leverage,
    panel_v, solved_v, sketch_v, design_v, prior_v,
    acc, part_tx, part_rx, right_tx, right_last, right_first,
    w_rx, w_split, y_tx, y_last, z_tx, z_all, s_tx, y_first,
    y_half, prod_tx, prod_rx, held, sol_tx, sol_rx, wide, design_own,
    load_sem, w_send, w_recv, send_sem, pair_send, recv_sem, wide_send, wide_recv,
):
    r = lax.axis_index("rows")
    c = lax.axis_index("cols")
    peer = 1 - c
    q = n // 4
    plane, p = r // q, r % q
    bottom, upper = plane // 2, plane % 2
    depth = panel.shape[1]
    lead = depth // LEAD
    step = (depth - lead) // CHUNKS
    k, pr = sketch.shape
    ir = pr // 2
    kh = k // PARTS
    width = inverses.shape[2]
    rows_here = prior.shape[1]

    def span_of(i):
        if i is None:
            return pl.ds(0, lead)
        return pl.ds(pl.multiple_of(lead + i * step, 128), step)

    def chunk(i):
        at = span_of(i)
        i = CHUNKS if i is None else i
        return (
            pltpu.make_async_copy(panel.at[:, at], panel_v.at[:, at], load_sem.at[0, i]),
            pltpu.make_async_copy(solved.at[:, at], solved_v.at[:, at], load_sem.at[1, i]),
        )

    for i in (None, *range(CHUNKS)):
        for copy in chunk(i):
            copy.start()
    late = [
        pltpu.make_async_copy(src, dst, load_sem.at[2, i])
        for i, (src, dst) in enumerate(((sketch, sketch_v), (prior, prior_v), (design, design_v)))
    ]

    barrier = pltpu.get_barrier_semaphore()

    def greet(to, core):
        pl.semaphore_signal(
            barrier, inc=1, device_id=(to, core), device_id_type=pl.DeviceIdType.MESH
        )

    @pl.when(c == 0)
    def _():
        greet(r, 1)

        @pl.when(r == 0)
        def _():
            def solvers(i, carry):
                greet(q + i, 1)
                return carry

            lax.fori_loop(0, 2 * q, solvers, 0)

    @pl.when(c == 1)
    def _():
        def column(i, carry):
            greet(i * q + p, 0)
            return carry

        def others(i, carry):
            greet((r + 1 + i) % n, 1)
            return carry

        lax.fori_loop(0, 4, column, 0)
        lax.fori_loop(0, n - 1, others, 0)


    def gathered(i):
        for copy in chunk(i):
            copy.wait()
        at = span_of(i)
        return nt(split(solved_v[:, at]), split(panel_v[:, at]))

    def body(i, carry):
        acc[...] += gathered(i)
        return carry

    def remote(src, dst, to, core, sent, recv):
        return pltpu.make_async_remote_copy(
            src_ref=src,
            dst_ref=dst,
            send_sem=sent,
            recv_sem=recv,
            device_id=(to, core),
            device_id_type=pl.DeviceIdType.MESH,
        )

    def put(src, dst, to, core, sent, recv):
        here = jnp.logical_and(to == r, core == c)

        @pl.when(here)
        def _():
            pltpu.make_async_copy(src, dst, recv).start()

        @pl.when(jnp.logical_not(here))
        def _():
            remote(src, dst, to, core, sent, recv).start()

    def settle(src, dst, to, core, sent, recv):
        here = jnp.logical_and(to == r, core == c)

        @pl.when(jnp.logical_not(here))
        def _():
            remote(src, dst, to, core, sent, recv).wait_send()

    def arrived(ref, recv):
        pltpu.make_async_copy(ref, ref, recv).wait()

    def weights(act, which):
        src = (inverses.at[1], coupling, inverses.at[0])[which]
        rows_at = pl.ds(pl.multiple_of(ir * upper, ir), ir)

        def move(skip):
            size = width - skip
            cols_at = pl.ds(pl.multiple_of(width * c + skip, skip or width), size)
            act(
                src.at[:, skip:],
                w_rx.at[which, rows_at, cols_at],
                (1 + bottom) * q + p,
                1,
                w_send.at[which],
                w_recv.at[which, upper, c],
            )

        if which == 1:
            move(0)
        else:

            @pl.when(jnp.logical_and(c == bottom, upper == 1))
            def _():
                move(width // 2)

            @pl.when(jnp.logical_or(c > bottom, jnp.logical_and(c == bottom, upper == 0)))
            def _():
                move(0)

    def bulk():
        weights(put, 0)
        weights(put, 1)

    early = jnp.logical_or(c == 0, plane >= 2)
    inner = jnp.logical_or(plane == 1, plane == 2)

    def meet():
        pl.semaphore_wait(barrier, jnp.where(c == 0, 4, jnp.where(inner, n + 1, n)))
        bulk()

    late[0].start()
    pl.when(plane == 3)(meet)
    acc[...] = gathered(None)
    lax.fori_loop(0, EARLY, body, 0)
    pl.when(jnp.logical_and(early, plane < 3))(meet)
    lax.fori_loop(EARLY, CHUNKS, body, 0)
    pl.when(jnp.logical_not(early))(meet)
    total = acc[...]
    share = (total[:k, :pr] + total[k:, :pr]) + (total[:k, pr:] + total[k:, pr:])

    def to_peer(src, dst, which, recv):
        return remote(src, dst, r, peer, pair_send.at[which], recv_sem.at[recv, 0])

    part_copy = to_peer(part_tx, part_rx, 0, 3)
    prod_copy = to_peer(prod_tx, prod_rx, 1, 0)
    sol_copy = to_peer(sol_tx, sol_rx, 2, 1)

    def group(g):
        return slice(g * width, (g + 1) * width)

    passes = [to_peer(y_first.at[:, group(g)], y_first.at[:, group(g)], 3 + g, 9 + g) for g in range(2)]
    slab = rows_here // SLABS

    def widen(i):
        at = pl.ds(pl.multiple_of(slab * i, slab), slab)
        return remote(wide.at[at], wide.at[at], r, 1, wide_send.at[i], wide_recv.at[i])

    lane = lax.broadcasted_iota(jnp.int32, (k, pr), 1)

    def fold(a, b, odd):
        even_half = jnp.where(lane < ir, a, pltpu.roll(b, ir, 1))
        odd_half = jnp.where(lane < ir, pltpu.roll(a, ir, 1), b)
        return jnp.where(odd, odd_half, even_half)

    def natural(ref, t):
        at = (t // q) * q + (2 * t) % q
        a = ref[:, pl.ds(pl.multiple_of(at * pr, pr), pr)]
        b = ref[:, pl.ds(pl.multiple_of((at + 1) * pr, pr), pr)]
        return fold(a, b, (t % q) // (q // 2) == 1)

    def round_group(ref, g):
        for t in range(g * q, (g + 1) * q):
            at = g * q + (2 * t) % q
            a = ref[:, at * pr : (at + 1) * pr]
            b = ref[:, (at + 1) * pr : (at + 2) * pr]
            if (t % q) // (q // 2) == 1:
                both = jnp.where(lane < ir, pltpu.roll(a, ir, 1), b)
            else:
                both = jnp.where(lane < ir, a, pltpu.roll(b, ir, 1))
            y_half[:, t * pr : (t + 1) * pr] = both.astype(jnp.bfloat16)

    def product(which):
        return nt(y_half[...], design_v[which * rows_here : (which + 1) * rows_here, :])

    def finish(g, weights_of):
        round_group(y_first, g)
        held[...] += nt(y_half[:, group(g)], weights_of[:rows_here, group(g)])

    def conclude():
        total_here = held[...]
        out_leverage[...] = jnp.mean(total_here * total_here, axis=0, keepdims=True)

        @pl.when(plane < 2)
        def _():
            out_solution[...] = natural(y_first, r % (2 * q))

    def piece(h):
        return pl.ds(pl.multiple_of((h * q + p) * pr, pr), pr)

    def near(i):
        return (p + 1 + i) % q

    def mixed(i, count):
        planes = count // q
        return (1 + i % planes) * q + near(i // planes)

    def spread(act, span, src, dst, cols_at, where, core, phase, part):
        rows_at = slice(part * kh, (part + 1) * kh)

        def one(i, carry):
            to = (mixed(i, span[1]), where(i // q) * q + near(i), where(i // q) * q + near(i), i)[phase]
            sent = send_sem.at[phase, part, i]
            recv = recv_sem.at[4 + phase if phase < 3 else 7 + bottom, part]
            act(src.at[rows_at], dst.at[rows_at, cols_at], to, core, sent, recv)
            return carry

        lax.fori_loop(*span, one, 0)

    last_at = pl.ds(pl.multiple_of(pr * (r % (2 * q)), pr), pr)

    def spread_last(act):
        def send(planes):
            for part in range(PARTS):
                spread(act, (0, planes * q), right_tx, right_last, last_at, lambda s: 1 + s, 1, 0, part)

        @pl.when(plane == 3)
        def _():
            send(2)

        @pl.when(plane == 2)
        def _():
            send(1)

    def spread_first(act):
        @pl.when(plane < 2)
        def _():
            for i in range(2):
                j = 2 * r + i
                to = (1 + j // (2 * q)) * q + j % q
                act(right_tx, right_first.at[(j % (2 * q)) // q], to, 1, send_sem.at[0, 0, i], recv_sem.at[2, 0])

    def spread_y_last(act, part, span):
        def where(s):
            return jnp.where(s == 0, 3 - plane, jnp.where(s == 1, plane, 3 * s - 6))

        spread(act, span, y_tx, y_last, piece(bottom), where, 1, 1, part)

    def spread_z(act, part):
        @pl.when(plane == 2)
        def _():
            spread(act, (0, 2 * q), z_tx, z_all, piece(1), lambda s: 1 + s, 1, 2, part)

        @pl.when(plane == 1)
        def _():
            spread(act, (0, q), z_tx, z_all, piece(0), lambda s: 1 + s, 1, 2, part)

    def spread_y_first(act, part):
        at = piece(bottom)
        act(s_tx, y_first.at[:, at], 0, 0, pair_send.at[5], recv_sem.at[9 + bottom, 0])
        spread(act, (0, n), s_tx, y_first, at, lambda s: s, 1, 3, part)

    def here(ref, phase, part, lo=0):
        arrived(ref.at[part * kh : (part + 1) * kh, lo:], recv_sem.at[4 + phase, part])

    def prepare(which, lo):
        size = 2 * width - lo
        x = w_rx[which, :, lo:]
        if which:
            wide = lax.broadcasted_iota(jnp.int32, (pr, pr), 1)
            blocks = []
            for base in range(0, size, width):
                for at in range(q):
                    i = base + (at // 2) * pr
                    j = i + width // 2
                    a, b = x[:, i : i + pr], x[:, j : j + pr]
                    if at % 2:
                        blocks.append(jnp.where(wide < ir, pltpu.roll(a, ir, 1), b))
                    else:
                        blocks.append(jnp.where(wide < ir, a, pltpu.roll(b, ir, 1)))
            x = jnp.concatenate(blocks, axis=1)
        w_split[which, :, lo:] = split(x)

    def ready(which, lo):
        skip = width // 2 if which != 1 else 0
        if skip:
            w_rx[which, ir:, lo : lo + skip] = jnp.zeros((ir, skip), jnp.float32)
        for core in range(lo // width, 2):
            for up in range(2):
                first = width * core + (skip if up == 1 and width * core == lo else 0)
                arrived(
                    w_rx.at[which, ir * up : ir * up + ir, first : width * core + width],
                    w_recv.at[which, up, core],
                )
        prepare(which, lo)

    def times(ref, which, part, lo):
        terms = nt(split(ref[part * kh : (part + 1) * kh, lo:]), w_split[which, :, lo:])
        terms = terms[:kh] + terms[kh:]
        return terms[:, :pr] + terms[:, pr:]

    @pl.when(c == 0)
    def _():
        part_tx[...] = share
        part_copy.start()
        weights(put, 2)
        late[1].start()
        late[2].start()
        late[0].wait()
        late[1].wait()
        late[2].wait()

        def share_slab(i, carry):
            at = pl.ds(pl.multiple_of(slab * i, slab), slab)
            theirs = pl.ds(pl.multiple_of(rows_here + slab * i, slab), slab)
            wide[at, :] = design_v[theirs, :].astype(jnp.float32)
            widen(i).start()
            return carry

        lax.fori_loop(0, SLABS, share_slab, 0)
        arrived(prod_rx, recv_sem.at[0, 0])
        held[...] = prod_rx[...] + prior_v[...]

        @pl.when(plane >= 2)
        def _():
            arrived(sol_rx, recv_sem.at[1, 0])
            out_solution[...] = sol_rx[...]

        for g in (1, 0):
            arrived(y_first.at[:, group(g)], recv_sem.at[9 + g, 0])
            finish(g, design_v)
        conclude()
        part_copy.wait_send()

        def sent_slab(i, carry):
            widen(i).wait_send()
            return carry

        lax.fori_loop(0, SLABS, sent_slab, 0)

    @pl.when(c == 1)
    def _():
        late[0].wait()
        own = sketch_v[...] - share
        arrived(part_rx, recv_sem.at[3, 0])
        right_tx[...] = own - part_rx[...]
        spread_last(put)
        spread_first(put)
        weights(put, 2)
        late[1].start()
        late[2].start()

        def solve(lo):
            ready(0, lo)
            for part in range(PARTS):
                here(right_last, 0, part, lo)
                y_tx[part * kh : (part + 1) * kh] = times(right_last, 0, part, lo)
                spread_y_last(put, part, (0, 2 * q))
            for part in range(PARTS):
                spread_y_last(put, part, (2 * q, n))
            ready(1, 0)
            arrived(right_first, recv_sem.at[2, 0])
            z_tx[...] = fold(right_first[0], right_first[1], p % 2 == 1)
            for part in range(PARTS):
                at = slice(part * kh, (part + 1) * kh)
                here(y_last, 1, part)
                z_tx[at] = z_tx[at] - times(y_last, 1, part, 0)
                spread_z(put, part)
            ready(2, lo)
            for part in range(PARTS):
                here(z_all, 2, part, lo)
                s_tx[part * kh : (part + 1) * kh] = times(z_all, 2, part, lo)
                spread_y_first(put, part)

        @pl.when(plane == 1)
        def _():
            solve(0)

        @pl.when(plane == 2)
        def _():
            solve(width)

        @pl.when(jnp.logical_not(inner))
        def _():
            for part in range(PARTS):
                here(y_last, 1, part)

        late[1].wait()
        late[2].wait()
        for g in range(2):
            round_group(y_last, g)
        prod_tx[...] = product(0)
        prod_copy.start()
        held[...] = product(1) + prior_v[...]

        @pl.when(plane >= 2)
        def _():
            mine = natural(y_last, r % (2 * q))
            sol_tx[...] = mine
            sol_copy.start()
            out_solution[...] = mine

        def narrow_slab(i, carry):
            at = pl.ds(pl.multiple_of(slab * i, slab), slab)
            arrived(wide.at[at], wide_recv.at[i])
            design_own[at, :] = wide[at, :].astype(jnp.bfloat16)
            return carry

        lax.fori_loop(0, SLABS, narrow_slab, 0)
        for g in (1, 0):
            arrived(y_first.at[:, group(g)], recv_sem.at[7 + g, 0])
            pl.when(r > 0)(passes[g].start)
            finish(g, design_own)
        conclude()
        spread_last(settle)
        spread_first(settle)

        @pl.when(inner)
        def _():
            for part in range(PARTS):
                spread_y_last(settle, part, (0, n))
                spread_z(settle, part)
                spread_y_first(settle, part)

        prod_copy.wait_send()
        for copy in passes:
            pl.when(r > 0)(copy.wait_send)

        @pl.when(plane >= 2)
        def _():
            sol_copy.wait_send()

    for which in range(3):
        weights(settle, which)


def emit(solution_v, leverage_v, out_solution, out_leverage, sem):
    copies = [
        pltpu.make_async_copy(solution_v, out_solution, sem.at[0]),
        pltpu.make_async_copy(leverage_v, out_leverage, sem.at[1]),
    ]
    for copy in copies:
        copy.start()
    for copy in copies:
        copy.wait()


def pinned(x):
    return pltpu.with_memory_space_constraint(x, pltpu.HBM)


def fused(n, panel, solved, sketch, inverses, coupling, design, prior):
    k = sketch.shape[1]
    pr, depth = panel.shape
    rows_here = prior.shape[0]
    width = inverses.shape[2]
    f32 = jnp.float32
    out_solution, out_leverage = pl.pallas_call(
        functools.partial(kernel, n),
        out_shape=(
            jax.ShapeDtypeStruct((k, pr), f32),
            jax.ShapeDtypeStruct((1, rows_here), f32),
        ),
        in_specs=[pl.BlockSpec(memory_space=pltpu.HBM)] * 7,
        out_specs=[pl.BlockSpec(memory_space=pltpu.VMEM)] * 2,
        scratch_shapes=[
            pltpu.VMEM((pr, depth), f32),
            pltpu.VMEM((k, depth), f32),
            pltpu.VMEM((k, pr), f32),
            pltpu.VMEM(design.shape, design.dtype),
            pltpu.VMEM((k, rows_here), f32),
            pltpu.VMEM((2 * k, 2 * pr), f32),
            pltpu.VMEM((k, pr), f32),
            pltpu.VMEM((k, pr), f32),
            pltpu.VMEM((k, pr), f32),
            pltpu.VMEM((k, 2 * width), f32),
            pltpu.VMEM((2, k, pr), f32),
            pltpu.VMEM((3, pr, 2 * width), f32),
            pltpu.VMEM((3, 2 * pr, 2 * width), jnp.bfloat16),
            pltpu.VMEM((k, pr), f32),
            pltpu.VMEM((k, 2 * width), f32),
            pltpu.VMEM((k, pr), f32),
            pltpu.VMEM((k, 2 * width), f32),
            pltpu.VMEM((k, pr), f32),
            pltpu.VMEM((k, 2 * width), f32),
            pltpu.VMEM((k, 2 * width), jnp.bfloat16),
            pltpu.VMEM((k, rows_here), f32),
            pltpu.VMEM((k, rows_here), f32),
            pltpu.VMEM((k, rows_here), f32),
            pltpu.VMEM((k, pr), f32),
            pltpu.VMEM((k, pr), f32),
            pltpu.VMEM((rows_here, design.shape[1]), f32),
            pltpu.VMEM((rows_here, design.shape[1]), design.dtype),
            pltpu.SemaphoreType.DMA((3, CHUNKS + 1)),
            pltpu.SemaphoreType.DMA((3,)),
            pltpu.SemaphoreType.DMA((3, 2, 2)),
            pltpu.SemaphoreType.DMA((4, PARTS, n)),
            pltpu.SemaphoreType.DMA((6,)),
            pltpu.SemaphoreType.DMA((11, PARTS)),
            pltpu.SemaphoreType.DMA((SLABS,)),
            pltpu.SemaphoreType.DMA((SLABS,)),
        ],
        compiler_params=pltpu.CompilerParams(
            collective_id=0, has_side_effects=True, vmem_limit_bytes=36 * 1024 * 1024
        ),
    )(*map(pinned, (panel, solved.T, sketch.T, inverses, coupling, design, prior.T)))
    out_solution, out_leverage = pl.pallas_call(
        emit,
        out_shape=(
            jax.ShapeDtypeStruct((k, pr), f32),
            jax.ShapeDtypeStruct((1, rows_here), f32),
        ),
        in_specs=[pl.BlockSpec(memory_space=pltpu.VMEM)] * 2,
        out_specs=[pl.BlockSpec(memory_space=pltpu.HBM)] * 2,
        scratch_shapes=[pltpu.SemaphoreType.DMA((2,))],
    )(*(pltpu.with_memory_space_constraint(x, pltpu.VMEM) for x in (out_solution, out_leverage)))
    return out_solution.T, out_leverage.reshape(rows_here)


def assemble(term):
    rows_here = lax.psum(term, "cols")
    return lax.all_gather(rows_here, "rows", axis=0, tiled=True)


def local(panel, solved, sketch, inverses, coupling, design, prior):
    highest = lax.Precision.HIGHEST
    partial_value = jnp.dot(panel, solved, precision=highest)
    local_right = sketch - lax.psum(partial_value, "cols")
    right = lax.all_gather(local_right, "rows", axis=0, tiled=True)
    blocks = right.shape[0] // 2
    width = inverses.shape[2]
    column = lax.axis_index("cols")
    offset = column * width

    def piece(vector):
        return lax.dynamic_slice_in_dim(vector, offset, width, 0)

    right_first = right[:blocks]
    right_last = right[blocks:]
    sketch_cols = right.shape[1]
    inverse_full = lax.all_gather(inverses[0], "cols", axis=1, tiled=True)
    coupling_full = lax.all_gather(coupling, "rows", axis=0, tiled=True)
    mixed = jnp.dot(inverse_full, coupling_full, precision=highest)
    term_last = jnp.dot(inverses[1], piece(right_last), precision=highest)
    term_first = jnp.dot(inverses[0], piece(right_first), precision=highest)
    joined = assemble(jnp.concatenate([term_last, term_first], axis=1))
    y_last = joined[:, :sketch_cols]
    partial_first = joined[:, sketch_cols:]
    correction = assemble(jnp.dot(mixed, piece(y_last), precision=highest))
    y_first = partial_first - correction
    solution = jnp.concatenate([y_first, y_last], axis=0)
    own_rows = sketch.shape[0]
    block_solution = lax.dynamic_slice_in_dim(
        solution, lax.axis_index("rows") * own_rows, own_rows, 0
    )
    design_cols = design.shape[1]
    rounded = lax.dynamic_slice_in_dim(solution, column * design_cols, design_cols, 0).astype(
        jnp.bfloat16
    )
    mine = lax.psum_scatter(
        jnp.dot(design, rounded, preferred_element_type=jnp.float32),
        "cols",
        scatter_dimension=0,
        tiled=True,
    )
    product = prior + mine
    leverage = jnp.mean(product * product, axis=1)
    return (block_solution, leverage)


def local_or_fused(rows, panel, solved, sketch, inverses, coupling, design, prior):
    args = (panel, solved, sketch, inverses, coupling, design, prior)
    pr, depth = panel.shape
    fits = pr == 128 and depth % (LEAD * 128) == 0 and (depth - depth // LEAD) % (CHUNKS * 128) == 0 and sketch.shape[1] % 32 == 0
    return fused(rows, *args) if fits else local(*args)


def solution(mesh):
    in_specs = (
        P("rows", "cols"),
        P("cols", None),
        P("rows", None),
        P(None, "rows", "cols"),
        P("rows", "cols"),
        P("rows", "cols"),
        P(("rows", "cols"), None),
    )
    out_specs = (P("rows", None), P(("rows", "cols")))
    rows, cols = mesh.shape["rows"], mesh.shape["cols"]
    step = local
    if cols == 2 and rows % 8 == 0:
        step = functools.partial(local_or_fused, rows)
    return jax.shard_map(step, mesh=mesh, in_specs=in_specs, out_specs=out_specs, check_vma=False)
```
